32 devices in a mesh: section: 2 (over x), tp: 16 (over z, y, core).
Axes of the slice: x: 2, y: 2, z: 4, core: 2. Of those that a mesh axis runs over, the one named last changes fastest.
Arguments:
- states: float32 [2, 128, 4096], P('section', 'tp'), may hold values from -6 to 6
- text_embed: bfloat16 [1, 128, 4096], P(None, 'tp'), may hold values from -6 to 6
- visual_embed: bfloat16 [1, 128, 4096], P(None, 'tp'), may hold values from -6 to 6
- prefix_len: int32 [1, 4], replicated, may hold values from 1 to 31
- segment_ids: int32 [3, 128], replicated, may hold values from 0 to 3, never falling along the last dimension, each value on 1 to 64 neighbouring positions
- gain: float32 [2, 4096], P('section'), may hold values from 0.25 to 1.75
- w_query: bfloat16 [2, 4096, 2048], P('section', None, 'tp'), may hold values from -0.5625 to 0.5625
- w_keyval: bfloat16 [2, 4096, 2048], P('section', None, 'tp'), may hold values from -0.5625 to 0.5625
- w_out: bfloat16 [2, 2048, 4096], P('section', 'tp'), may hold values from -0.5 to 0.5
Outputs:
- section_out: float32 [2, 2, 128, 4096], P(None, 'section', 'tp')
The draws below stay inside these ranges and needn't reach their ends.
All inputs are finite; a program needn't handle non-finite values.
Results may differ from the reference program's by a relative error of at most 0.028.
Values may be sent and summed in bfloat16 or wider, within the bound.
A program may use at most 64 MiB of HBM per device.

```python
import math
import jax
import jax.numpy as jnp
import numpy as np
from jax import lax

D = 4096
HEAD = 64
Q_PER = 2
SEGS = 4
WINDOW = 2
MB_TOK = 128
HEADS = 32
KV_HEADS = 16
NEW = 1
CHAIN = 3
N_SECTION = 2
N_TP = 16


def draw_w_query(key, part):
    spread = D ** (-0.5)
    fresh = jax.random.normal(jax.random.fold_in(key, 23), (N_SECTION, D, KV_HEADS, Q_PER, HEAD), jnp.float32) * spread
    fresh = jnp.clip(fresh, -36.0 * spread, 36.0 * spread)
    return fresh.reshape(N_SECTION, D, HEADS * HEAD).astype(jnp.bfloat16)


def draw_w_keyval(key, part):
    spread = D ** (-0.5)
    fresh = jax.random.normal(jax.random.fold_in(key, 37), (N_SECTION, D, KV_HEADS, 2, HEAD), jnp.float32) * spread
    fresh = jnp.clip(fresh, -36.0 * spread, 36.0 * spread)
    return fresh.reshape(N_SECTION, D, KV_HEADS * 2 * HEAD).astype(jnp.bfloat16)


def with_ends(values, own_key, low, largest):
    index_at = [jax.random.randint(jax.random.fold_in(own_key, axis), (), 0, length) for axis, length in enumerate(values.shape)]
    widest = values.shape.index(max(values.shape))
    next_to = index_at[:widest] + [(index_at[widest] + 1) % values.shape[widest]] + index_at[widest + 1:]
    return values.at[tuple(index_at)].set(low).at[tuple(next_to)].set(largest)


def steps_of(rng, dims, pieces, low, top_value):
    level = 1.0
    for dim, shards_of in pieces:
        steps = jax.random.uniform(jax.random.fold_in(jax.random.fold_in(rng, 6), dim), (shards_of,), jnp.float32, low / len(pieces), top_value / len(pieces))
        level = level * jnp.repeat(jnp.exp(steps), dims[dim] // shards_of).reshape((-1,) + (1,) * (len(dims) - 1 - dim))
    return level


def profile(amount, total, bound, lean):
    weights = [(1 << 20) // math.isqrt(rank ** lean) + 1 for rank in range(2, amount + 1)]
    rest, holding = total - bound - (amount - 1), [1] * (amount - 1)
    while rest > 0:
        free = [i for i in range(amount - 1) if holding[i] < bound]
        mass, budget = sum([weights[i] for i in free]), rest
        for i in free:
            extra = min(bound - holding[i], max(1, budget * weights[i] // mass), rest)
            holding[i] = holding[i] + extra
            rest = rest - extra
    return np.array([bound] + holding)


def uneven(own_key, number_of, total, limit, lean):
    if number_of == 2:
        one = jax.random.randint(own_key, (), max(1, total - limit), min(limit, total - 1) + 1)
        return jnp.stack([one, total - one])
    sizes = jnp.asarray(profile(number_of, total, limit, lean), jnp.int32)
    twos = (number_of - 1) // 2
    giver, taker = sizes[1:1 + 2 * twos:2], sizes[2:2 + 2 * twos:2]
    margin = jnp.minimum(giver - 1, limit - taker)
    passed = jax.random.randint(jax.random.fold_in(own_key, 1), (twos,), 0, 1 << 20) % (margin + 1)
    sizes = sizes.at[1:1 + 2 * twos:2].set(giver - passed).at[2:2 + 2 * twos:2].set(taker + passed)
    return sizes[jax.random.permutation(jax.random.fold_in(own_key, 2), number_of)]


def bell_draw(stream_key, shape, deviation, most, shards=(), kind=jnp.bfloat16):
    entries = jax.random.normal(stream_key, shape, jnp.float32) * deviation
    if len(shards) > 0:
        entries = steps_of(stream_key, shape, shards, -0.22, 0.18) * entries
    return jnp.clip(entries, min=-most, max=most).astype(kind)


def setup_inputs(seed: int = 0) -> dict:
    arg_keys = jax.random.split(jax.random.key(seed), 10)
    return {
        "states": bell_draw(arg_keys[0], (N_SECTION, MB_TOK, D), 1.0, 6.0, ((0, 2), (1, 16)), jnp.float32),
        "text_embed": bell_draw(arg_keys[1], (NEW, MB_TOK, D), 1.0, 6.0, ((1, 16),)),
        "visual_embed": bell_draw(arg_keys[2], (NEW, MB_TOK, D), 1.0, 6.0, ((1, 16),)),
        "prefix_len": with_ends(jax.random.randint(arg_keys[3], (NEW, SEGS), 1, MB_TOK // 4), jax.random.fold_in(arg_keys[3], 1), 1, (MB_TOK // 4) - 1).astype(jnp.int32),
        "segment_ids": jax.vmap(lambda own: jnp.searchsorted(jnp.cumsum(uneven(own, SEGS, MB_TOK, MB_TOK // 2, 2)), jnp.arange(MB_TOK), side="right"))(jax.random.split(arg_keys[4], CHAIN)).reshape((CHAIN, MB_TOK)).astype(jnp.int32),
        "gain": jnp.clip(1.0 + 0.15 * jax.random.normal(arg_keys[5], (N_SECTION, D), jnp.float32), 0.25, 1.75),
        "w_query": draw_w_query(jax.random.fold_in(arg_keys[9], 71), 0),
        "w_keyval": draw_w_keyval(jax.random.fold_in(arg_keys[9], 71), 0),
        "w_out": bell_draw(arg_keys[8], (N_SECTION, HEADS * HEAD, D), (Q_PER * HEAD) ** -0.5, 0.5, ((0, 2), (1, 16))),
    }


norm_eps = 1e-05
rope_base = 500000.0

def seg_offsets(seg_row):
    earlier = (seg_row[None, :] < seg_row[:, None]).astype(jnp.int32)
    first_pos = lax.optimization_barrier(jnp.sum(earlier, axis=1)).astype(jnp.int32)
    return jnp.arange(seg_row.shape[0], dtype=jnp.int32) - first_pos

def rotate(values, offsets):
    half_dim = values.shape[-1] // 2
    inv_freq = rope_base ** (-(jnp.arange(half_dim, dtype=jnp.float32) * 2.0) / values.shape[-1])
    angles = offsets.astype(jnp.float32)[:, None] * inv_freq[None, :]
    view_shape = (values.shape[0],) + (1,) * (values.ndim - 2) + (half_dim,)
    cosine = jnp.cos(angles).reshape(view_shape)
    sine_part = jnp.sin(angles).reshape(view_shape)
    front_half = values[..., :half_dim]
    back_half = values[..., half_dim:]
    return jnp.concatenate([front_half * cosine - back_half * sine_part, back_half * cosine + front_half * sine_part], axis=-1)

def rms_normed(rows, gain_row):
    scale = lax.rsqrt(lax.optimization_barrier(jnp.mean(rows * rows, axis=-1, keepdims=True)) + norm_eps)
    return rows * scale * gain_row

def reference(states, text_embed, visual_embed, prefix_len, segment_ids, gain, w_query, w_keyval, w_out):

    def apply_layer(residual, section_num, seg_row):
        normed = rms_normed(residual, gain[section_num]).astype(jnp.bfloat16)
        queries = jnp.dot(normed, w_query[section_num], preferred_element_type=jnp.float32).reshape(MB_TOK, HEADS, HEAD)
        keyval = jnp.dot(normed, w_keyval[section_num], preferred_element_type=jnp.float32).reshape(MB_TOK, KV_HEADS, 2, HEAD)
        offsets = seg_offsets(seg_row)
        queries = rotate(queries, offsets).astype(jnp.bfloat16)
        key_rows = rotate(keyval[:, :, 0], offsets).astype(jnp.bfloat16)
        value_rows = keyval[:, :, 1].astype(jnp.bfloat16)
        key_rows = jnp.repeat(key_rows, Q_PER, axis=1)
        value_rows = jnp.repeat(value_rows, Q_PER, axis=1)
        scores = jnp.einsum('qhd,khd->hqk', queries.astype(jnp.float32), key_rows.astype(jnp.float32)) * HEAD ** (-0.5)
        position = jnp.arange(MB_TOK, dtype=jnp.int32)
        allowed = (seg_row[None, :] == seg_row[:, None]) & (position[None, :] <= position[:, None])
        scores = jnp.where(allowed[None], scores, -1e+30)
        weights = jax.nn.softmax(scores, axis=-1).astype(jnp.bfloat16)
        mixed_heads = jnp.einsum('hqk,khd->qhd', weights.astype(jnp.float32), value_rows.astype(jnp.float32)).astype(jnp.bfloat16)
        grouped = mixed_heads.reshape(MB_TOK, N_TP, Q_PER * HEAD)
        out_grouped = w_out[section_num].reshape(N_TP, Q_PER * HEAD, D)
        partial_value = jnp.einsum('tgc,gcd->gtd', grouped.astype(jnp.float32), out_grouped.astype(jnp.float32)).astype(jnp.bfloat16)
        return residual + lax.optimization_barrier(jnp.sum(partial_value.astype(jnp.float32), axis=0))

    def embed_batch(batch_num):
        seg_row = segment_ids[N_SECTION + batch_num]
        offsets = seg_offsets(seg_row)
        onehot = seg_row[:, None] == jnp.arange(SEGS, dtype=jnp.int32)[None, :]
        prefix_cap = lax.optimization_barrier(jnp.sum(jnp.where(onehot, prefix_len[batch_num][None, :], 0), axis=1))
        is_visual = offsets < prefix_cap
        return jnp.where(is_visual[:, None], visual_embed[batch_num], text_embed[batch_num]).astype(jnp.float32)
    outputs = []
    current = [states[section_num] for section_num in range(N_SECTION)]
    results = current
    for step_num in range(WINDOW):
        if step_num > 0:
            current = [embed_batch(step_num - 1)] + results[:-1]
        results = [apply_layer(current[section_num], section_num, segment_ids[step_num - section_num + N_SECTION - 1]) for section_num in range(N_SECTION)]
        outputs.append(jnp.stack(results))
    return jnp.stack(outputs)
```

```python
import functools
import math

import jax
import jax.numpy as jnp
from jax import lax
from jax.experimental import pallas as pl
from jax.experimental.pallas import tpu as pltpu
from jax.sharding import PartitionSpec as P

HEAD = 64
WINDOW = 2
NORM_EPS = 1e-05
ROPE_BASE = 500000.0
MESH = pl.DeviceIdType.MESH
F32 = jnp.float32
BF16 = jnp.bfloat16

MID = 2
INNER = 2
CHUNKS = 4


def iota(shape, dim):
    return lax.broadcasted_iota(jnp.int32, shape, dim)


def kernel(
    sections, ranks,
    states, text, visual, prefix, seg_in, gain_in, wq_in, wkv_in, wo_in,
    out,
    st_v, tx_v, vi_v, seg_v, g_v, w_v, wo_v, res, xg, xf, mix, acc,
    csend, crecv, bsend, brecv, asend, arecv, hsend, hrecv,
    load_sem, ag_send, ag_recv, c_sem, b_sem, a_send, a_recv, h_sem,
):
    s = lax.axis_index("section")
    r = lax.axis_index("tp")
    outer = ranks // (MID * INNER)
    c = lax.rem(r, INNER)
    b = lax.rem(r // INNER, MID)
    a = r // (INNER * MID)
    bp, cp = 1 - b, 1 - c
    rows = st_v.shape[0]
    depth = st_v.shape[1]
    total = rows * ranks
    qcols = wq_in.shape[2]
    kvcols = wkv_in.shape[2]
    cw = depth // CHUNKS

    def rank(ai, bi, ci):
        return (ai * MID + bi) * INNER + ci

    loads = [
        pltpu.make_async_copy(src, dst, load_sem.at[i])
        for i, (src, dst) in enumerate([
            (states.at[0], st_v),
            (gain_in, g_v),
            (seg_in, seg_v),
            (wq_in.at[0], w_v.at[:, pl.ds(0, qcols)]),
            (wkv_in.at[0], w_v.at[:, pl.ds(qcols, kvcols)]),
            (wo_in.at[0], wo_v),
            (text.at[0], tx_v),
            (visual.at[0], vi_v),
        ])
    ]
    for load in loads:
        load.start()

    outer_peers = [lax.rem(a + d, outer) for d in range(1, outer)]
    tp_peers = [rank(ai, b, c) for ai in outer_peers] + [rank(a, bp, c), rank(a, b, cp)]
    barrier = pltpu.get_barrier_semaphore()
    for peer in tp_peers:
        pl.semaphore_signal(barrier, inc=1, device_id={"tp": peer}, device_id_type=MESH)

    @pl.when(s > 0)
    def _():
        pl.semaphore_signal(barrier, inc=1, device_id={"section": s - 1}, device_id_type=MESH)

    @pl.when(s < sections - 1)
    def _():
        pl.semaphore_signal(barrier, inc=1, device_id={"section": s + 1}, device_id_type=MESH)

    loads[0].wait()
    loads[1].wait()
    loads[2].wait()

    def start_row(seg_row, seg_col):
        return jnp.sum(jnp.where(seg_row < seg_col, 1.0, 0.0), axis=1, keepdims=True)

    def column_of(seg_row, count, base):
        shape = (count, total)
        here = iota(shape, 1) == iota(shape, 0) + base
        return jnp.sum(jnp.where(here, seg_row, 0.0), axis=1, keepdims=True)

    def normed(value):
        scale = lax.rsqrt(jnp.mean(value * value, axis=-1, keepdims=True) + NORM_EPS)
        return (value * scale * g_v[...]).astype(BF16)

    sends = []

    def remote(src, dst, send_sem, recv_sem, **where):
        return pltpu.make_async_remote_copy(
            src_ref=src, dst_ref=dst, send_sem=send_sem, recv_sem=recv_sem,
            device_id=where, device_id_type=MESH,
        )

    lane = iota((total, qcols), 1)

    for t in range(WINDOW):
        if t == 0:
            res[...] = st_v[...]
        else:
            seg_row = seg_v[sections + t - 1 : sections + t, :].astype(F32)

            @pl.when(s == 0)
            def _():
                loads[6].wait()
                loads[7].wait()
                own = column_of(seg_row, rows, r * rows)
                cap = jnp.zeros_like(own)
                for d in range(prefix.shape[1]):
                    cap = cap + jnp.where(own == float(d), prefix[t - 1, d].astype(F32), 0.0)
                pos = (iota((rows, 1), 0) + r * rows).astype(F32)
                seen = pos - start_row(seg_row, own) < cap
                res[...] = jnp.where(seen, vi_v[...].astype(F32), tx_v[...].astype(F32))

            @pl.when(s > 0)
            def _():
                loads[6].wait()
                loads[7].wait()
                for k in range(CHUNKS):
                    remote(
                        hsend.at[k], hrecv.at[k], h_sem.at[0, k], h_sem.at[1, k], section=s - 1
                    ).wait_recv()
                    res[:, k * cw : (k + 1) * cw] = hrecv[k].astype(F32)

        xg[t, r] = normed(res[...])
        if t == 0:
            beside = jnp.minimum(s, 1) + jnp.minimum(sections - 1 - s, 1)
            pl.semaphore_wait(barrier, len(tp_peers) + beside)

        used = [0]

        def block(q, peer):
            copy = remote(
                xg.at[t, q], xg.at[t, q], ag_send.at[t, used[0]], ag_recv.at[t, q], tp=peer
            )
            used[0] += 1
            copy.start()
            sends.append(copy)

        def arrived(q):
            remote(
                xg.at[t, q], xg.at[t, q], ag_send.at[t, 0], ag_recv.at[t, q], tp=rank(a, b, cp)
            ).wait_recv()

        for ai in outer_peers:
            block(r, rank(ai, b, c))
        block(r, rank(a, bp, c))
        block(r, rank(a, b, cp))

        seg_here = seg_v[pl.ds(t - s + sections - 1, 1), :].astype(F32)
        seg_col = column_of(seg_here, total, 0)
        offset = iota((total, 1), 0).astype(F32) - start_row(seg_here, seg_col)
        half = HEAD // 2
        m = lax.rem(lane, half).astype(F32)
        freq = jnp.exp(m * (-2.0 / HEAD * math.log(ROPE_BASE)))
        angle = offset * freq
        cosine = jnp.cos(angle)
        front = lax.rem(lane, HEAD) < half
        sine = jnp.where(front, -jnp.sin(angle), jnp.sin(angle))
        allowed = (seg_here == seg_col) & (iota((total, total), 1) <= iota((total, total), 0))

        forward = [lax.rem(a - d + outer, outer) for d in range(1, outer)]
        for ai in forward:
            q = rank(ai, b, c)
            arrived(q)
            block(q, rank(a, bp, c))
            block(q, rank(a, b, cp))
        for ai in [a] + forward:
            q = rank(ai, bp, c)
            arrived(q)
            block(q, rank(a, b, cp))
        for ai in [a] + forward:
            for bi in (b, bp):
                arrived(rank(ai, bi, cp))

        for i in range(ranks // 2):
            xf[i * 2 * rows : (i + 1) * 2 * rows, :] = jnp.concatenate(
                [xg[t, 2 * i].astype(F32), xg[t, 2 * i + 1].astype(F32)], axis=0
            ).astype(BF16)
        if t == 0:
            loads[3].wait()
            loads[4].wait()
        mapped = jnp.dot(xf[...], w_v[...], preferred_element_type=F32)

        def rotate(value):
            swapped = jnp.where(
                front, pltpu.roll(value, qcols - half, 1), pltpu.roll(value, half, 1)
            )
            return value * cosine + swapped * sine

        queries = rotate(mapped[:, :qcols])
        keyval = mapped[:, qcols:]
        keys = rotate(keyval)
        first = lane < HEAD
        keys = jnp.where(first, keys, pltpu.roll(keys, HEAD, 1)).astype(BF16)
        values = jnp.where(first, pltpu.roll(keyval, HEAD, 1), keyval).astype(BF16)
        mixed = jnp.zeros((total, qcols), F32)
        for h in range(qcols // HEAD):
            mine = lane // HEAD == h
            scores = lax.dot_general(
                jnp.where(mine, queries, 0.0).astype(BF16), keys,
                (((1,), (1,)), ((), ())), preferred_element_type=F32,
            ) * HEAD ** (-0.5)
            scores = jnp.where(allowed, scores, -1e30)
            top = jnp.max(scores, axis=-1, keepdims=True)
            grown = jnp.exp(scores - top)
            probs = (grown / jnp.sum(grown, axis=-1, keepdims=True)).astype(BF16)
            mixed = jnp.where(mine, jnp.dot(probs, values, preferred_element_type=F32), mixed)
        for ci in range(INNER):
            mix[ci] = jnp.concatenate(
                [
                    mixed[rank(ai, bi, ci) * rows : (rank(ai, bi, ci) + 1) * rows]
                    for bi in range(MID) for ai in range(outer)
                ],
                axis=0,
            ).astype(BF16)
        if t == 0:
            loads[5].wait()

        def chunk(k):
            return slice(k * cw, (k + 1) * cw)

        def stage1(k):
            theirs = jnp.dot(mix[cp], wo_v[:, chunk(k)], preferred_element_type=F32)
            for i in range(MID * outer):
                csend[t, k, i // outer, i % outer] = theirs[i * rows : (i + 1) * rows].astype(BF16)
            copy = remote(
                csend.at[t, k], crecv.at[t, k], c_sem.at[0, t, k], c_sem.at[1, t, k],
                tp=rank(a, b, cp),
            )
            copy.start()
            sends.append(copy)
            mine = jnp.dot(mix[c], wo_v[:, chunk(k)], preferred_element_type=F32)
            for i in range(MID * outer):
                acc[k, i // outer, i % outer] = mine[i * rows : (i + 1) * rows]
            return copy

        def stage2(k, copy):
            copy.wait_recv()
            for ai in range(outer):
                bsend[t, k, ai] = (acc[k, bp, ai] + crecv[t, k, bp, ai].astype(F32)).astype(BF16)
            copy = remote(
                bsend.at[t, k], brecv.at[t, k], b_sem.at[0, t, k], b_sem.at[1, t, k],
                tp=rank(a, bp, c),
            )
            copy.start()
            sends.append(copy)
            return copy

        def held(k, ai):
            return (
                acc[k, b, ai] + crecv[t, k, b, ai].astype(F32) + brecv[t, k, ai].astype(F32)
            )

        def stage3(k, copy):
            copy.wait_recv()
            copies = []
            for d, ai in enumerate(outer_peers):
                asend[t, k, d] = held(k, ai).astype(BF16)
                copy = remote(
                    asend.at[t, k, d], arecv.at[t, k, d],
                    a_send.at[t, k, d], a_recv.at[t, k, d], tp=rank(ai, b, c),
                )
                copy.start()
                sends.append(copy)
                copies.append(copy)
            return copies

        def stage4(k, copies):
            summed = held(k, a)
            for d, copy in enumerate(copies):
                copy.wait_recv()
                summed = summed + arecv[t, k, d].astype(F32)
            value = res[:, chunk(k)] + summed
            out[t, 0, :, chunk(k)] = value
            if t < WINDOW - 1:
                hsend[k] = value.astype(BF16)

                @pl.when(s < sections - 1)
                def _():
                    remote(
                        hsend.at[k], hrecv.at[k], h_sem.at[0, k], h_sem.at[1, k], section=s + 1
                    ).start()

        one, two, three = {}, {}, {}
        for step in range(CHUNKS + 3):
            if step < CHUNKS:
                one[step] = stage1(step)
            if 0 <= step - 1 < CHUNKS:
                two[step - 1] = stage2(step - 1, one[step - 1])
            if 0 <= step - 2 < CHUNKS:
                three[step - 2] = stage3(step - 2, two[step - 2])
            if 0 <= step - 3 < CHUNKS:
                stage4(step - 3, three[step - 3])

    for copy in sends:
        copy.wait_send()

    @pl.when(s < sections - 1)
    def _():
        for k in range(CHUNKS):
            remote(
                hsend.at[k], hrecv.at[k], h_sem.at[0, k], h_sem.at[1, k], section=s + 1
            ).wait_send()


def body(sections, ranks, states, text, visual, prefix, seg, gain, wq, wkv, wo):
    rows, depth = states.shape[1:]
    total = rows * ranks
    outer = ranks // (MID * INNER)
    cw = depth // CHUNKS
    qcols, kvcols = wq.shape[2], wkv.shape[2]
    hbm = pl.BlockSpec(memory_space=pl.ANY)
    dma = pltpu.SemaphoreType.DMA
    return pl.pallas_call(
        functools.partial(kernel, sections, ranks),
        out_shape=jax.ShapeDtypeStruct((WINDOW, 1, rows, depth), F32),
        in_specs=[hbm, hbm, hbm, pl.BlockSpec(memory_space=pltpu.SMEM)] + [hbm] * 5,
        out_specs=pl.BlockSpec(memory_space=pltpu.VMEM),
        scratch_shapes=[
            pltpu.VMEM((rows, depth), F32),
            pltpu.VMEM((rows, depth), BF16),
            pltpu.VMEM((rows, depth), BF16),
            pltpu.VMEM(seg.shape, jnp.int32),
            pltpu.VMEM((1, depth), F32),
            pltpu.VMEM((depth, qcols + kvcols), BF16),
            pltpu.VMEM((qcols, depth), BF16),
            pltpu.VMEM((rows, depth), F32),
            pltpu.VMEM((WINDOW, ranks, rows, depth), BF16),
            pltpu.VMEM((total, depth), BF16),
            pltpu.VMEM((INNER, total // INNER, qcols), BF16),
            pltpu.VMEM((CHUNKS, MID, outer, rows, cw), F32),
            pltpu.VMEM((WINDOW, CHUNKS, MID, outer, rows, cw), BF16),
            pltpu.VMEM((WINDOW, CHUNKS, MID, outer, rows, cw), BF16),
            pltpu.VMEM((WINDOW, CHUNKS, outer, rows, cw), BF16),
            pltpu.VMEM((WINDOW, CHUNKS, outer, rows, cw), BF16),
            pltpu.VMEM((WINDOW, CHUNKS, outer - 1, rows, cw), BF16),
            pltpu.VMEM((WINDOW, CHUNKS, outer - 1, rows, cw), BF16),
            pltpu.VMEM((CHUNKS, rows, cw), BF16),
            pltpu.VMEM((CHUNKS, rows, cw), BF16),
            dma((8,)),
            dma((WINDOW, ranks - 1)),
            dma((WINDOW, ranks)),
            dma((2, WINDOW, CHUNKS)),
            dma((2, WINDOW, CHUNKS)),
            dma((WINDOW, CHUNKS, outer - 1)),
            dma((WINDOW, CHUNKS, outer - 1)),
            dma((2, CHUNKS)),
        ],
        compiler_params=pltpu.CompilerParams(
            collective_id=0, has_side_effects=True, vmem_limit_bytes=56 * 1024 * 1024
        ),
        name="relay",
    )(states, text, visual, prefix, seg, gain, wq, wkv, wo)


def solution(mesh):
    sizes = dict(mesh.shape)
    return jax.shard_map(
        functools.partial(body, sizes["section"], sizes["tp"]),
        mesh=mesh,
        in_specs=(
            P("section", "tp", None),
            P(None, "tp", None),
            P(None, "tp", None),
            P(),
            P(),
            P("section", None),
            P("section", None, "tp"),
            P("section", None, "tp"),
            P("section", "tp", None),
        ),
        out_specs=P(None, "section", "tp", None),
        check_vma=False,
    )
```

```python
import functools
import math

import jax
import jax.numpy as jnp
from jax import lax
from jax.experimental import pallas as pl
from jax.experimental.pallas import tpu as pltpu
from jax.sharding import PartitionSpec as P

HEAD = 64
WINDOW = 2
NORM_EPS = 1e-05
ROPE_BASE = 500000.0
MESH = pl.DeviceIdType.MESH
F32 = jnp.float32
BF16 = jnp.bfloat16

MID = 2
INNER = 2
CHUNKS = 8
PIECES = 2
LAG_ADD = 5
LAG_MID = 3


def iota(shape, dim):
    return lax.broadcasted_iota(jnp.int32, shape, dim)


def kernel(
    sections, ranks,
    states, text, visual, prefix, seg_in, gain_in, wq_in, wkv_in, wo_in,
    out,
    st_v, tx_v, vi_v, seg_v, g_v, w_v, wo_v, res, xg, xf, mix, acc,
    csend, crecv, bsend, brecv, asend, arecv, hsend, hrecv,
    load_sem, ag_send, ag_recv, c_sem, b_sem, a_send, a_recv, h_sem,
):
    s = lax.axis_index("section")
    r = lax.axis_index("tp")
    outer = ranks // (MID * INNER)
    c = lax.rem(r, INNER)
    b = lax.rem(r // INNER, MID)
    a = r // (INNER * MID)
    bp, cp = 1 - b, 1 - c
    rows = st_v.shape[0]
    depth = st_v.shape[1]
    total = rows * ranks
    qcols = wq_in.shape[2]
    kvcols = wkv_in.shape[2]
    cw = depth // CHUNKS
    pw = depth // PIECES

    def rank(ai, bi, ci):
        return (ai * MID + bi) * INNER + ci

    loads = [
        pltpu.make_async_copy(src, dst, load_sem.at[i])
        for i, (src, dst) in enumerate([
            (states.at[0], st_v),
            (gain_in, g_v),
            (seg_in, seg_v),
            (wq_in.at[0], w_v.at[:, pl.ds(0, qcols)]),
            (wkv_in.at[0], w_v.at[:, pl.ds(qcols, kvcols)]),
            (wo_in.at[0], wo_v),
            (text.at[0], tx_v),
            (visual.at[0], vi_v),
        ])
    ]
    for load in loads:
        load.start()

    if outer == 4:
        flip = a + 1 - 2 * lax.rem(a, 2)
        outer_peers = [flip, 3 - flip, 3 - a]
        outer_from = outer_peers
    else:
        outer_peers = [lax.rem(a + d, outer) for d in range(1, outer)]
        outer_from = [lax.rem(a - d + outer, outer) for d in range(1, outer)]
    tp_peers = [rank(ai, b, c) for ai in outer_peers] + [rank(a, bp, c), rank(a, b, cp)]
    barrier = pltpu.get_barrier_semaphore()
    for peer in tp_peers:
        pl.semaphore_signal(barrier, inc=1, device_id={"tp": peer}, device_id_type=MESH)

    @pl.when(s > 0)
    def _():
        pl.semaphore_signal(barrier, inc=1, device_id={"section": s - 1}, device_id_type=MESH)

    @pl.when(s < sections - 1)
    def _():
        pl.semaphore_signal(barrier, inc=1, device_id={"section": s + 1}, device_id_type=MESH)

    loads[0].wait()
    loads[1].wait()
    loads[2].wait()

    def start_row(seg_row, seg_col):
        return jnp.sum(jnp.where(seg_row < seg_col, 1.0, 0.0), axis=1, keepdims=True)

    def column_of(seg_row, count, base):
        shape = (count, total)
        here = iota(shape, 1) == iota(shape, 0) + base
        return jnp.sum(jnp.where(here, seg_row, 0.0), axis=1, keepdims=True)

    def normed(value):
        scale = lax.rsqrt(jnp.mean(value * value, axis=-1, keepdims=True) + NORM_EPS)
        return (value * scale * g_v[...]).astype(BF16)

    sends = []

    def remote(src, dst, send_sem, recv_sem, **where):
        return pltpu.make_async_remote_copy(
            src_ref=src, dst_ref=dst, send_sem=send_sem, recv_sem=recv_sem,
            device_id=where, device_id_type=MESH,
        )

    lane = iota((total, qcols), 1)

    for t in range(WINDOW):
        if t == 0:
            res[...] = st_v[...]
        else:
            seg_row = seg_v[sections + t - 1 : sections + t, :].astype(F32)

            @pl.when(s == 0)
            def _():
                loads[6].wait()
                loads[7].wait()
                own = column_of(seg_row, rows, r * rows)
                cap = jnp.zeros_like(own)
                for d in range(prefix.shape[1]):
                    cap = cap + jnp.where(own == float(d), prefix[t - 1, d].astype(F32), 0.0)
                pos = (iota((rows, 1), 0) + r * rows).astype(F32)
                seen = pos - start_row(seg_row, own) < cap
                res[...] = jnp.where(seen, vi_v[...].astype(F32), tx_v[...].astype(F32))

            @pl.when(s > 0)
            def _():
                loads[6].wait()
                loads[7].wait()
                for k in range(CHUNKS):
                    remote(
                        hsend.at[k], hrecv.at[k], h_sem.at[0, k], h_sem.at[1, k], section=s - 1
                    ).wait_recv()
                    res[:, k * cw : (k + 1) * cw] = hrecv[k].astype(F32)

        mine = normed(res[...])
        for p in range(PIECES):
            xg[t, p, r] = mine[:, p * pw : (p + 1) * pw]
        if t == 0:
            beside = jnp.minimum(s, 1) + jnp.minimum(sections - 1 - s, 1)
            pl.semaphore_wait(barrier, len(tp_peers) + beside)

        used = [0]

        def block(p, q, peer):
            copy = remote(
                xg.at[t, p, q], xg.at[t, p, q],
                ag_send.at[t, used[0]], ag_recv.at[t, p, q], tp=peer,
            )
            used[0] += 1
            copy.start()
            sends.append(copy)

        def arrived(p, q):
            remote(
                xg.at[t, p, q], xg.at[t, p, q],
                ag_send.at[t, 0], ag_recv.at[t, p, q], tp=rank(a, b, cp),
            ).wait_recv()

        for p in range(PIECES):
            block(p, r, rank(a, bp, c))
            for ai in outer_peers:
                block(p, r, rank(ai, b, c))
            block(p, r, rank(a, b, cp))

        seg_here = seg_v[pl.ds(t - s + sections - 1, 1), :].astype(F32)
        seg_col = column_of(seg_here, total, 0)
        offset = iota((total, 1), 0).astype(F32) - start_row(seg_here, seg_col)
        half = HEAD // 2
        m = lax.rem(lane, half).astype(F32)
        freq = jnp.exp(m * (-2.0 / HEAD * math.log(ROPE_BASE)))
        angle = offset * freq
        cosine = jnp.cos(angle)
        front = lax.rem(lane, HEAD) < half
        sine = jnp.where(front, -jnp.sin(angle), jnp.sin(angle))
        allowed = (seg_here == seg_col) & (iota((total, total), 1) <= iota((total, total), 0))

        hops = [(p, d) for p in range(PIECES) for d in range(outer)]
        from_a = [a] + outer_from
        for i in range(len(hops) + LAG_MID):
            if i < len(hops) and hops[i][1] > 0:
                p, d = hops[i]
                q = rank(from_a[d], b, c)
                arrived(p, q)
                block(p, q, rank(a, bp, c))
                block(p, q, rank(a, b, cp))
            if i >= LAG_MID:
                p, d = hops[i - LAG_MID]
                q = rank(from_a[d], bp, c)
                arrived(p, q)
                block(p, q, rank(a, b, cp))
        if t == 0:
            loads[3].wait()
            loads[4].wait()
        mapped = None
        for p in range(PIECES):
            for ai in from_a:
                for bi in (b, bp):
                    arrived(p, rank(ai, bi, cp))
            cols = slice(p * pw, (p + 1) * pw)
            for i in range(ranks // 2):
                xf[i * 2 * rows : (i + 1) * 2 * rows, cols] = jnp.concatenate(
                    [xg[t, p, 2 * i].astype(F32), xg[t, p, 2 * i + 1].astype(F32)], axis=0
                ).astype(BF16)
            part = jnp.dot(xf[:, cols], w_v[cols, :], preferred_element_type=F32)
            mapped = part if mapped is None else mapped + part

        def rotate(value):
            swapped = jnp.where(
                front, pltpu.roll(value, qcols - half, 1), pltpu.roll(value, half, 1)
            )
            return value * cosine + swapped * sine

        queries = rotate(mapped[:, :qcols])
        keyval = mapped[:, qcols:]
        keys = rotate(keyval)
        first = lane < HEAD
        keys = jnp.where(first, keys, pltpu.roll(keys, HEAD, 1)).astype(BF16)
        values = jnp.where(first, pltpu.roll(keyval, HEAD, 1), keyval).astype(BF16)
        mixed = jnp.zeros((total, qcols), F32)
        for h in range(qcols // HEAD):
            mine = lane // HEAD == h
            scores = lax.dot_general(
                jnp.where(mine, queries, 0.0).astype(BF16), keys,
                (((1,), (1,)), ((), ())), preferred_element_type=F32,
            ) * HEAD ** (-0.5)
            scores = jnp.where(allowed, scores, -1e30)
            top = jnp.max(scores, axis=-1, keepdims=True)
            grown = jnp.exp(scores - top)
            probs = (grown / jnp.sum(grown, axis=-1, keepdims=True)).astype(BF16)
            mixed = jnp.where(mine, jnp.dot(probs, values, preferred_element_type=F32), mixed)
        for ci in range(INNER):
            mix[ci] = jnp.concatenate(
                [
                    mixed[rank(ai, bi, ci) * rows : (rank(ai, bi, ci) + 1) * rows]
                    for bi in range(MID) for ai in range(outer)
                ],
                axis=0,
            ).astype(BF16)
        if t == 0:
            loads[5].wait()

        def chunk(k):
            return slice(k * cw, (k + 1) * cw)

        def stage1(k):
            theirs = jnp.dot(mix[cp], wo_v[:, chunk(k)], preferred_element_type=F32)
            for i in range(MID * outer):
                csend[t, k, i // outer, i % outer] = theirs[i * rows : (i + 1) * rows].astype(BF16)
            copy = remote(
                csend.at[t, k], crecv.at[t, k], c_sem.at[0, t, k], c_sem.at[1, t, k],
                tp=rank(a, b, cp),
            )
            copy.start()
            sends.append(copy)
            mine = jnp.dot(mix[c], wo_v[:, chunk(k)], preferred_element_type=F32)
            for i in range(MID * outer):
                acc[k, i // outer, i % outer] = mine[i * rows : (i + 1) * rows]
            return copy

        def stage2(k, copy):
            copy.wait_recv()
            for ai in range(outer):
                bsend[t, k, ai] = (acc[k, bp, ai] + crecv[t, k, bp, ai].astype(F32)).astype(BF16)
            copy = remote(
                bsend.at[t, k], brecv.at[t, k], b_sem.at[0, t, k], b_sem.at[1, t, k],
                tp=rank(a, bp, c),
            )
            copy.start()
            sends.append(copy)
            return copy

        def held(k, ai):
            return (
                acc[k, b, ai] + crecv[t, k, b, ai].astype(F32) + brecv[t, k, ai].astype(F32)
            )

        def stage3(k, copy):
            copy.wait_recv()
            copies = []
            for d, ai in enumerate(outer_peers):
                asend[t, k, d] = held(k, ai).astype(BF16)
                copy = remote(
                    asend.at[t, k, d], arecv.at[t, k, d],
                    a_send.at[t, k, d], a_recv.at[t, k, d], tp=rank(ai, b, c),
                )
                copy.start()
                sends.append(copy)
                copies.append(copy)
            return copies

        def stage4(k, copies):
            summed = held(k, a)
            for d, copy in enumerate(copies):
                copy.wait_recv()
                summed = summed + arecv[t, k, d].astype(F32)
            value = res[:, chunk(k)] + summed
            out[t, 0, :, chunk(k)] = value
            if t < WINDOW - 1:
                hsend[k] = value.astype(BF16)

                @pl.when(s < sections - 1)
                def _():
                    remote(
                        hsend.at[k], hrecv.at[k], h_sem.at[0, k], h_sem.at[1, k], section=s + 1
                    ).start()

        one, two, three = {}, {}, {}
        for k in range(CHUNKS + 1):
            if k < CHUNKS:
                one[k] = stage1(k)
            if k > 0:
                two[k - 1] = stage2(k - 1, one[k - 1])
        for k in range(CHUNKS + LAG_ADD):
            if k < CHUNKS:
                three[k] = stage3(k, two[k])
            if k >= LAG_ADD:
                stage4(k - LAG_ADD, three[k - LAG_ADD])

    for copy in sends:
        copy.wait_send()

    @pl.when(s < sections - 1)
    def _():
        for k in range(CHUNKS):
            remote(
                hsend.at[k], hrecv.at[k], h_sem.at[0, k], h_sem.at[1, k], section=s + 1
            ).wait_send()


def body(sections, ranks, states, text, visual, prefix, seg, gain, wq, wkv, wo):
    rows, depth = states.shape[1:]
    total = rows * ranks
    outer = ranks // (MID * INNER)
    cw = depth // CHUNKS
    qcols, kvcols = wq.shape[2], wkv.shape[2]
    hbm = pl.BlockSpec(memory_space=pl.ANY)
    dma = pltpu.SemaphoreType.DMA
    return pl.pallas_call(
        functools.partial(kernel, sections, ranks),
        out_shape=jax.ShapeDtypeStruct((WINDOW, 1, rows, depth), F32),
        in_specs=[hbm, hbm, hbm, pl.BlockSpec(memory_space=pltpu.SMEM)] + [hbm] * 5,
        out_specs=pl.BlockSpec(memory_space=pltpu.VMEM),
        scratch_shapes=[
            pltpu.VMEM((rows, depth), F32),
            pltpu.VMEM((rows, depth), BF16),
            pltpu.VMEM((rows, depth), BF16),
            pltpu.VMEM(seg.shape, jnp.int32),
            pltpu.VMEM((1, depth), F32),
            pltpu.VMEM((depth, qcols + kvcols), BF16),
            pltpu.VMEM((qcols, depth), BF16),
            pltpu.VMEM((rows, depth), F32),
            pltpu.VMEM((WINDOW, PIECES, ranks, rows, depth // PIECES), BF16),
            pltpu.VMEM((total, depth), BF16),
            pltpu.VMEM((INNER, total // INNER, qcols), BF16),
            pltpu.VMEM((CHUNKS, MID, outer, rows, cw), F32),
            pltpu.VMEM((WINDOW, CHUNKS, MID, outer, rows, cw), BF16),
            pltpu.VMEM((WINDOW, CHUNKS, MID, outer, rows, cw), BF16),
            pltpu.VMEM((WINDOW, CHUNKS, outer, rows, cw), BF16),
            pltpu.VMEM((WINDOW, CHUNKS, outer, rows, cw), BF16),
            pltpu.VMEM((WINDOW, CHUNKS, outer - 1, rows, cw), BF16),
            pltpu.VMEM((WINDOW, CHUNKS, outer - 1, rows, cw), BF16),
            pltpu.VMEM((CHUNKS, rows, cw), BF16),
            pltpu.VMEM((CHUNKS, rows, cw), BF16),
            dma((8,)),
            dma((WINDOW, PIECES * (ranks - 1))),
            dma((WINDOW, PIECES, ranks)),
            dma((2, WINDOW, CHUNKS)),
            dma((2, WINDOW, CHUNKS)),
            dma((WINDOW, CHUNKS, outer - 1)),
            dma((WINDOW, CHUNKS, outer - 1)),
            dma((2, CHUNKS)),
        ],
        compiler_params=pltpu.CompilerParams(
            collective_id=0, has_side_effects=True, vmem_limit_bytes=56 * 1024 * 1024
        ),
        name="relay",
    )(states, text, visual, prefix, seg, gain, wq, wkv, wo)


def solution(mesh):
    sizes = dict(mesh.shape)
    return jax.shard_map(
        functools.partial(body, sizes["section"], sizes["tp"]),
        mesh=mesh,
        in_specs=(
            P("section", "tp", None),
            P(None, "tp", None),
            P(None, "tp", None),
            P(),
            P(),
            P("section", None),
            P("section", None, "tp"),
            P("section", None, "tp"),
            P("section", "tp", None),
        ),
        out_specs=P(None, "section", "tp", None),
        check_vma=False,
    )
```
